32 devices in a mesh: seq: 8 (over z, y), batch: 4 (over x, core).
Axes of the slice: x: 2, y: 2, z: 4, core: 2. Of those that a mesh axis runs over, the one named last changes fastest.
Arguments:
- coarse_act: bfloat16 [8, 512, 1536], P('batch', 'seq'), may hold values from -6 to 6
- skip_act: bfloat16 [8, 1024, 1536], P('batch', 'seq'), may hold values from -6 to 6
- proj_in: bfloat16 [1536, 1536], P('seq'), may hold values from -0.15625 to 0.15625
- proj_out: bfloat16 [1536, 1536], P('seq'), may hold values from -0.15625 to 0.15625
- depth_kernel: float32 [3, 1536], replicated, may hold values from -3.5 to 3.5
- norm_gain: float32 [1536], replicated, may hold values from 0.5 to 1.5
- grad_out: bfloat16 [8, 1024, 1536], P('batch', 'seq'), may hold values from -6 to 6
Outputs:
- block_out: bfloat16 [8, 1024, 1536], P('batch', 'seq')
- grad_coarse_act: bfloat16 [8, 512, 1536], P('batch', 'seq')
- grad_kernel: float32 [3, 1536], replicated
- grad_gain: float32 [1536], replicated
The draws below stay inside these ranges and needn't reach their ends.
All inputs are finite; a program needn't handle non-finite values.
Results may differ from the reference program's by a relative error of at most 0.012.
Values may be sent and summed in bfloat16 or wider, within the bound.
No kernel may reach another device: no remote copies, remote signals or barrier semaphores. Data moves between devices by JAX's collectives and lax.ppermute only.
A program may use at most 128 MiB of HBM per device.

```python
import jax
import jax.numpy as jnp
from jax import lax

C = 1536
BINS = 1024
COARSE = 512
SAMPLES = 8


def level_of(stream_key, shape, shards, least, largest):
    level = 1.0
    for position, shards_of in shards:
        steps = jax.random.uniform(jax.random.fold_in(jax.random.fold_in(stream_key, 6), position), (shards_of,), jnp.float32, least / len(shards), largest / len(shards))
        level = level * jnp.repeat(jnp.exp(steps), shape[position] // shards_of).reshape((-1,) + (1,) * (len(shape) - 1 - position))
    return level


def noise(key, extent, scale, limit, split=(), dtype=jnp.bfloat16):
    values = jax.random.normal(key, extent, jnp.float32) * scale
    if len(split) > 0:
        values = level_of(key, extent, split, -0.22, 0.18) * values
    return jnp.clip(values, min=-limit, max=limit).astype(dtype)


def setup_inputs(seed: int = 0) -> dict:
    splits = jax.random.split(jax.random.key(seed), 8)
    coarse_act = noise(splits[0], (SAMPLES, COARSE, C), 1.0, 6.0, ((0, 4), (1, 8)))
    skip_act = noise(splits[1], (SAMPLES, BINS, C), 1.0, 6.0, ((0, 4), (1, 8)))
    proj_in = noise(splits[2], (C, C), C ** -0.5, 0.15625, ((0, 8),))
    proj_out = noise(splits[3], (C, C), C ** -0.5, 0.15625, ((0, 8),))
    depth_kernel = noise(splits[4], (3, C), 3 ** -0.5, 3.5, (), jnp.float32)
    norm_gain = jnp.clip(1.0 + 0.1 * jax.random.normal(splits[5], (C,), jnp.float32), 0.5, 1.5)
    grad_out = noise(splits[6], (SAMPLES, BINS, C), 1.0, 6.0, ((0, 4), (1, 8)))
    return {"coarse_act": coarse_act, "skip_act": skip_act, "proj_in": proj_in, "proj_out": proj_out, "depth_kernel": depth_kernel, "norm_gain": norm_gain, "grad_out": grad_out}


epsilon = 1e-05

def norm_gelu(values_in, gain):
    values = values_in.astype(jnp.float32)
    average = lax.optimization_barrier(jnp.mean(values, axis=-1, keepdims=True))
    centered = values - average
    variance = lax.optimization_barrier(jnp.mean(centered * centered, axis=-1, keepdims=True))
    return jax.nn.gelu(centered * lax.rsqrt(variance + epsilon) * gain, approximate=False)

def one_sample(coarse_act, skip_act, grad_out, proj_in, proj_out, depth_kernel, norm_gain):
    activated = norm_gelu(coarse_act, norm_gain)
    act_low = activated.astype(jnp.bfloat16)
    coarse = jnp.dot(act_low, proj_in, preferred_element_type=jnp.float32).astype(jnp.bfloat16)
    merged = (jnp.repeat(coarse, 2, axis=0).astype(jnp.float32) + skip_act.astype(jnp.float32)).astype(jnp.bfloat16)
    padded = jnp.pad(merged, ((1, 1), (0, 0)))
    mixed = depth_kernel[0] * padded[:-2] + depth_kernel[1] * padded[1:-1] + depth_kernel[2] * padded[2:]
    mixed = mixed.astype(jnp.bfloat16)
    block_out = jnp.dot(mixed, proj_out, preferred_element_type=jnp.float32).astype(jnp.bfloat16)
    grad_mixed = jnp.dot(grad_out, proj_out.T, preferred_element_type=jnp.float32).astype(jnp.bfloat16)
    grad_wide = grad_mixed.astype(jnp.float32)
    grad_kernel = jnp.stack([lax.optimization_barrier(jnp.sum(padded[shift:shift + BINS].astype(jnp.float32) * grad_wide, axis=0)) for shift in range(3)])
    grad_pad = jnp.pad(grad_wide, ((1, 1), (0, 0)))
    grad_merged = depth_kernel[0] * grad_pad[2:] + depth_kernel[1] * grad_pad[1:-1] + depth_kernel[2] * grad_pad[:-2]
    grad_coarse = lax.optimization_barrier(jnp.sum(grad_merged.reshape(COARSE, 2, C), axis=1)).astype(jnp.bfloat16)
    grad_act = jnp.dot(grad_coarse, proj_in.T, preferred_element_type=jnp.float32)
    unused, pullback = jax.vjp(norm_gelu, coarse_act, norm_gain)
    grad_cur, grad_gain = pullback(grad_act)
    return (block_out, grad_cur.astype(jnp.bfloat16), grad_kernel, grad_gain)

def reference(coarse_act, skip_act, proj_in, proj_out, depth_kernel, norm_gain, grad_out):

    def step(items):
        return one_sample(items[0], items[1], items[2], proj_in, proj_out, depth_kernel, norm_gain)
    block_out, grad_cur, kernels, gains = lax.map(step, (coarse_act, skip_act, grad_out))
    return (block_out, grad_cur, lax.optimization_barrier(jnp.sum(kernels, axis=0)), lax.optimization_barrier(jnp.sum(gains, axis=0)))
```

```python
import functools

import jax
import jax.numpy as jnp
from jax import lax
from jax.experimental import pallas as pl
from jax.experimental.pallas import tpu as pltpu
from jax.sharding import PartitionSpec as P

epsilon = 1e-05
AXES = ("seq", "batch")
f32 = jnp.float32
bf16 = jnp.bfloat16
VMEM = pl.BlockSpec(memory_space=pltpu.VMEM)
SMEM = pl.BlockSpec(memory_space=pltpu.SMEM)
EXTRA = 16


class Grid:
    def __init__(self, mesh):
        self.seq, self.batch = mesh.shape["seq"], mesh.shape["batch"]
        self.ys = 2 if self.seq % 2 == 0 else 1
        self.zs = self.seq // self.ys
        self.cs = 2 if self.batch % 2 == 0 else 1
        self.xs = self.batch // self.cs

    def perm(self, to):
        pairs = []
        for i in range(self.seq * self.batch):
            s, b = divmod(i, self.batch)
            z, y, x, c = s // self.ys, s % self.ys, b // self.cs, b % self.cs
            z, y, x, c = to(z, y, x, c)
            pairs.append((i, (z * self.ys + y) * self.batch + x * self.cs + c))
        return pairs

    def send(self, value, to):
        return lax.ppermute(value, AXES, self.perm(to))

    def place(self):
        s, b = lax.axis_index("seq"), lax.axis_index("batch")
        return s // self.ys, s % self.ys, b // self.cs, b % self.cs

    def fits(self, rows):
        return self.ys == 2 and self.cs == 2 and self.xs == 2 and self.zs <= 4 and rows % 64 == 0


def next_z(grid):
    return lambda z, y, x, c: ((z + 1) % grid.zs, y, x, c)


def other_y(z, y, x, c):
    return z, 1 - y, x, c


def other_x(z, y, x, c):
    return z, y, 1 - x, c


def other_c(z, y, x, c):
    return z, y, x, 1 - c


def assemble(pieces, offsets, rows, width):
    def body(at, *refs):
        out = refs[-1]
        for i, ref in enumerate(refs[:-1]):
            out[pl.ds(pl.multiple_of(at[i], 16), ref.shape[0]), :] = ref[...]

    return pl.pallas_call(
        body,
        out_shape=jax.ShapeDtypeStruct((rows, width), bf16),
        in_specs=[SMEM] + [VMEM] * len(pieces),
        out_specs=VMEM,
        name="assemble",
    )(jnp.stack(offsets).astype(jnp.int32), *pieces)


def gather(grid, weights):
    rows, width = weights.shape
    if not grid.fits(rows):
        return lax.all_gather(weights, "seq", axis=0, tiled=True)
    z, y, x, c = grid.place()
    half, quarter = rows // 2, rows // 4
    ring = [lax.dynamic_slice_in_dim(weights, c * half, half, 0)]
    for _ in range(grid.zs - 1):
        ring.append(grid.send(ring[-1], next_z(grid)))
    ring = jnp.stack(ring)
    side = grid.send(lax.dynamic_slice_in_dim(ring, x * quarter, quarter, 1), other_y)
    far = grid.send(side, other_x)
    groups = [(ring, y, 0), (side, 1 - y, x * quarter), (far, 1 - y, (1 - x) * quarter)]
    pieces, offsets = [], []
    for data, y_at, inner in groups:
        for source, c_at in ((data, c), (grid.send(data, other_c), 1 - c)):
            for j in range(grid.zs):
                pieces.append(source[j])
                offsets.append((((z - j) % grid.zs) * 2 + y_at) * rows + c_at * half + inner)
    return assemble(pieces, offsets, rows * grid.seq, width)


def halves(skip, grad):
    samples, bins, width = skip.shape

    def body(skip_ref, grad_ref, skip_out, grad_out):
        row = lax.broadcasted_iota(jnp.int32, (bins, bins), 0)
        col = lax.broadcasted_iota(jnp.int32, (bins, bins), 1)
        half = bins // 2
        pick = jnp.where(col == jnp.where(row < half, 2 * row, 2 * (row - half) + 1), 1.0, 0.0)
        pick = pick.astype(bf16)
        for ref, out in ((skip_ref, skip_out), (grad_ref, grad_out)):
            for s in range(samples):
                both = jnp.dot(pick, ref[s], preferred_element_type=f32).astype(bf16)
                out[0, s * half : (s + 1) * half] = both[:half]
                out[1, s * half : (s + 1) * half] = both[half:]

    shape = jax.ShapeDtypeStruct((2, samples * bins // 2, width), bf16)
    return pl.pallas_call(
        body, out_shape=(shape, shape), in_specs=[VMEM, VMEM], out_specs=(VMEM, VMEM), name="halves"
    )(skip, grad)


def before(value, edges, samples):
    rows = value.shape[0] // samples
    at = lax.broadcasted_iota(jnp.int32, value.shape, 0)
    moved = pltpu.roll(value, 1, 0)
    for s in range(samples):
        moved = jnp.where(at == s * rows, edges[s : s + 1], moved)
    return moved


def after(value, edges, samples):
    rows = value.shape[0] // samples
    at = lax.broadcasted_iota(jnp.int32, value.shape, 0)
    moved = pltpu.roll(value, value.shape[0] - 1, 0)
    for s in range(samples):
        moved = jnp.where(at == (s + 1) * rows - 1, edges[samples + s : samples + s + 1], moved)
    return moved


def back_mid(grad_split, grad_edge, whole_out, kernel, samples, block):
    _, rows, width = grad_split.shape
    mid = whole_out.shape[0]
    dims = (((1,), (1,)), ((), ()))

    def body(g, edge, w, k, mixed_out, coarse_out):
        for n in range(0, mid, block):
            cols = slice(n, n + block)
            part = w[cols, :]

            def times(a):
                return lax.dot_general(a, part, dims, preferred_element_type=f32).astype(bf16)

            even, odd, ends = times(g[0]), times(g[1]), times(edge[...]).astype(f32)
            mixed_out[0, :, cols] = even
            mixed_out[1, :, cols] = odd
            even, odd = even.astype(f32), odd.astype(f32)
            odd_before, even_after = before(odd, ends, samples), after(even, ends, samples)
            coarse_out[:, cols] = (
                k[0:1, cols] * (odd + even_after)
                + k[1:2, cols] * (even + odd)
                + k[2:3, cols] * (odd_before + even)
            ).astype(bf16)

    return pl.pallas_call(
        body,
        out_shape=(
            jax.ShapeDtypeStruct((2, rows, mid), bf16),
            jax.ShapeDtypeStruct((rows, mid), bf16),
        ),
        in_specs=[VMEM] * 4,
        out_specs=(VMEM, VMEM),
        name="back_mid",
    )(grad_split, grad_edge, whole_out, kernel)


def finish(act, whole_in, skip_split, skip_edge, grad_mixed, grad_coarse, kernel, slope, unit, scale, gain, samples, block):
    _, rows, mid = skip_split.shape
    width = whole_in.shape[0]
    count = rows // samples
    dims = (((1,), (1,)), ((), ()))

    def body(a, w, skip, edge, gm, gc, k, d, xh, r, gn, mixed_out, cur_out, sums_out, held):
        row = lax.broadcasted_iota(jnp.int32, (2 * count, 2 * count), 0)
        col = lax.broadcasted_iota(jnp.int32, (2 * count, 2 * count), 1)
        order = jnp.where(row == jnp.where(col < count, 2 * col, 2 * (col - count) + 1), 1.0, 0.0)
        order = order.astype(bf16)
        for n in range(0, mid, block):
            cols = slice(n, n + block)
            coarse = jnp.dot(a[...], w[:, cols], preferred_element_type=f32).astype(bf16).astype(f32)
            ends = (coarse[rows:] + edge[:, cols].astype(f32)).astype(bf16).astype(f32)
            even = (coarse[:rows] + skip[0, :, cols].astype(f32)).astype(bf16).astype(f32)
            odd = (coarse[:rows] + skip[1, :, cols].astype(f32)).astype(bf16).astype(f32)
            odd_before, even_after = before(odd, ends, samples), after(even, ends, samples)
            g_even, g_odd = gm[0, :, cols].astype(f32), gm[1, :, cols].astype(f32)
            sums_out[0:1, cols] = jnp.sum(odd_before * g_even + even * g_odd, 0, keepdims=True)
            sums_out[1:2, cols] = jnp.sum(even * g_even + odd * g_odd, 0, keepdims=True)
            sums_out[2:3, cols] = jnp.sum(odd * g_even + even_after * g_odd, 0, keepdims=True)
            k0, k1, k2 = k[0:1, cols], k[1:2, cols], k[2:3, cols]
            m_even = (k0 * odd_before + k1 * even + k2 * odd).astype(bf16)
            m_odd = (k0 * even + k1 * odd + k2 * even_after).astype(bf16)
            for s in range(samples):
                take = slice(s * count, (s + 1) * count)
                both = jnp.concatenate([m_even[take], m_odd[take]], axis=0)
                both = jnp.dot(order, both, preferred_element_type=f32).astype(bf16)
                mixed_out[2 * s * count : 2 * (s + 1) * count, cols] = both
        first = jnp.zeros((rows, 1), f32)
        second = jnp.zeros((rows, 1), f32)
        for n in range(0, width, block):
            cols = slice(n, n + block)
            dn = lax.dot_general(gc[...], w[cols, :], dims, preferred_element_type=f32) * d[:, cols]
            hat = xh[:, cols]
            sums_out[3:4, cols] = jnp.sum(dn * hat, 0, keepdims=True)
            dn = dn * gn[0:1, cols]
            held[:, cols] = dn
            first = first + jnp.sum(dn, 1, keepdims=True)
            second = second + jnp.sum(dn * hat, 1, keepdims=True)
        first, second = first / width, second / width
        cur_out[...] = (r[...] * (held[...] - first - xh[...] * second)).astype(bf16)

    return pl.pallas_call(
        body,
        out_shape=(
            jax.ShapeDtypeStruct((2 * rows, mid), bf16),
            jax.ShapeDtypeStruct((rows, width), bf16),
            jax.ShapeDtypeStruct((4, mid), f32),
        ),
        in_specs=[VMEM] * 11,
        out_specs=(VMEM, VMEM, VMEM),
        scratch_shapes=[pltpu.VMEM((rows, width), f32)],
        name="finish",
    )(act, whole_in, skip_split, skip_edge, grad_mixed, grad_coarse, kernel, slope, unit, scale, gain)


def total(grid, value):
    for axis, size in (("batch", grid.batch), ("seq", grid.seq)):
        if size & (size - 1):
            value = lax.psum(value, axis)
            continue
        step = 1
        while step < size:
            value = value + lax.ppermute(value, axis, [(i, i ^ step) for i in range(size)])
            step *= 2
    return value


def edges_of(first, last, count):
    left = lax.ppermute(last, "seq", [(i, i + 1) for i in range(count - 1)])
    right = lax.ppermute(first, "seq", [(i + 1, i) for i in range(count - 1)])
    return left, right


def on_device(grid, coarse_act, skip_act, proj_in, proj_out, depth_kernel, norm_gain, grad_out):
    samples, bins, mid = coarse_act.shape[0], skip_act.shape[1], skip_act.shape[2]
    count, width = coarse_act.shape[1:]
    rows = samples * count
    block = 256 if mid % 256 == 0 and width % 256 == 0 else 128

    whole_out = gather(grid, proj_out)
    whole_in = gather(grid, proj_in)

    first = jnp.concatenate([coarse_act[:, 0], skip_act[:, 0], grad_out[:, 0]], axis=0)
    last = jnp.concatenate([coarse_act[:, -1], skip_act[:, -1], grad_out[:, -1]], axis=0)
    left, right = edges_of(first, last, grid.seq)

    def edge(i):
        take = slice(i * samples, (i + 1) * samples)
        got = jnp.concatenate([left[take], right[take]], axis=0)
        return jnp.pad(got, ((0, EXTRA - 2 * samples), (0, 0)))

    skip_split, grad_split = halves(skip_act, grad_out)

    values = coarse_act.reshape(rows, width)
    values = jnp.concatenate([values, edge(0)], axis=0).astype(f32)
    average = jnp.mean(values, axis=-1, keepdims=True)
    centered = values - average
    scale = lax.rsqrt(jnp.mean(centered * centered, axis=-1, keepdims=True) + epsilon)
    unit = centered * scale
    normed = unit * norm_gain
    act = jax.nn.gelu(normed, approximate=False).astype(bf16)
    own = normed[:rows]
    slope = 0.5 * (1.0 + lax.erf(own * 0.7071067811865476)) + own * (
        0.3989422804014327 * jnp.exp(-0.5 * own * own)
    )
    grad_mixed, grad_coarse = back_mid(grad_split, edge(2), whole_out, depth_kernel, samples, block)
    mixed, grad_cur, sums = finish(
        act, whole_in, skip_split, edge(1), grad_mixed, grad_coarse, depth_kernel,
        slope, unit[:rows], scale[:rows], norm_gain.reshape(1, width), samples, block,
    )
    sums = total(grid, sums)
    block_out = jnp.dot(mixed, whole_out, preferred_element_type=f32).astype(bf16)
    return (
        block_out.reshape(samples, bins, whole_out.shape[1]),
        grad_cur.reshape(samples, count, width),
        sums[:3],
        sums[3],
    )


def solution(mesh):
    spread = P("batch", "seq", None)
    in_specs = (spread, spread, P("seq", None), P("seq", None), P(), P(), spread)
    out_specs = (spread, spread, P(), P())
    return jax.shard_map(
        functools.partial(on_device, Grid(mesh)), mesh=mesh, in_specs=in_specs, out_specs=out_specs, check_vma=False
    )
```
